32 devices in a mesh: dp: 4 (over y, core), expert: 4 (over z), tensor: 2 (over x).
Axes of the slice: x: 2, y: 2, z: 4, core: 2. Of those that a mesh axis runs over, the one named last changes fastest.
Arguments:
- router_input: bfloat16 [1024, 2048], P(('dp', 'expert'), 'tensor'), may hold values from -6 to 6
- router_weight: bfloat16 [2048, 8], replicated, may hold values from -0.125 to 0.125
- expert_ids: int32 [1024, 2], P(('dp', 'expert', 'tensor')), may hold values from 0 to 7, all different within a row; in each aligned block of 32 rows (0 to 31, 32 to 63, ...) at most 9 rows name the same one
- down_weight: bfloat16 [61440, 2048], P(('expert', 'tensor')), may hold values from -0.0625 to 0.0625
- hidden: bfloat16 [4, 72, 61440], P('dp', None, ('expert', 'tensor')), may hold values from -6 to 6
- grad_output: bfloat16 [1024, 2048], P(('dp', 'expert', 'tensor')), may hold values from -4 to 4
Outputs:
- weight_grad: bfloat16 [61440, 2048], P(('expert', 'tensor', 'dp'))
- hidden_grad: bfloat16 [4, 72, 61440], P('dp', None, ('expert', 'tensor'))
- router_grad: float32 [2048, 8], replicated
- input_grad: bfloat16 [1024, 2048], P(('dp', 'expert', 'tensor'))
The draws below stay inside these ranges and needn't reach their ends.
Inputs may be any that keep to these rules, and one draw needn't show every extreme that they name: `expert_ids`: each row names 2 different experts. Within the 32 rows of one device no expert is named more than 9 times, and some device's rows name some expert exactly 9 times.
All inputs are finite; a program needn't handle non-finite values.
Results may differ from the reference program's by a relative error of at most 0.018.
Values may be sent and summed in bfloat16 or wider, within the bound.
No kernel may reach another device: no remote copies, remote signals or barrier semaphores. Data moves between devices by JAX's collectives and lax.ppermute only.
A program may use at most 192 MiB of HBM per device.

```python
import math
import jax
import jax.numpy as jnp
import numpy as np
from jax import lax

D = 2048
FF = 7680
EXPERTS = 8
TOPK = 2
TOK_DEV = 32
CAP = 9
SOURCES = 8
TOKENS = 1024
N_DP = 4


def shard_levels(key, shape, split, smallest, largest):
    level, own = 1.0, jax.random.fold_in(key, 6)
    for axis_at, blocks in split:
        draws = jnp.exp(jax.random.uniform(jax.random.fold_in(own, axis_at), (blocks,), jnp.float32, smallest / len(split), largest / len(split)))
        level = level * jnp.repeat(draws, shape[axis_at] // blocks).reshape([-1 if axis == axis_at else 1 for axis in range(len(shape))])
    return level


def deal_out(key, own, number, rows, amount, top, most, slope):
    order = jax.random.permutation(key, amount)
    crowded, common = shares(amount, rows * top, most, slope, True), shares(amount, rows * top, most, slope, False)
    places = jnp.arange(amount)

    def named(tallies, offset_by):
        used = int((tallies > 0).sum())
        fixed = max(1, used // 4)
        shifted = fixed + (places - fixed + offset_by * (used - fixed)) % max(1, amount - fixed)
        return jnp.zeros((amount,), jnp.int32).at[order[jnp.where(places < fixed, places, shifted)]].set(jnp.asarray(tallies, jnp.int32))

    tallies = jnp.where(number % 4 == 0, named(crowded, number // 4), named(common, number - number // 4 - 1))
    mixed = jax.random.permutation(jax.random.fold_in(own, 3), amount)
    donor, receiver = mixed[0:amount // 2 * 2:2], mixed[1:amount // 2 * 2:2]
    slack = jnp.minimum(tallies[donor] - 1, most - tallies[receiver]) // 2
    slack = jnp.where((donor == order[0]) | (receiver == order[0]) | (tallies[receiver] == 0), 0, jnp.maximum(slack, 0))
    shifted = jax.random.randint(jax.random.fold_in(own, 4), (amount // 2,), 0, 1 << 20) % (slack + 1)
    tallies = tallies.at[donor].add(-shifted).at[receiver].add(shifted)
    items = jnp.searchsorted(jnp.cumsum(tallies), jnp.arange(rows * top), side="right").astype(jnp.int32)
    listing = items.reshape(top, rows).T
    listing = listing[jax.random.permutation(jax.random.fold_in(own, 1), rows)]
    offset_by = jax.random.randint(jax.random.fold_in(own, 2), (rows, 1), 0, top)
    return jnp.take_along_axis(listing, (jnp.arange(top)[None, :] + offset_by) % top, axis=1)


def shares(count, total, bound, slope, full):
    weights = [(1 << 20) // math.isqrt(grade ** slope) + 1 for grade in range(1, count + 1)]
    largest = bound if full else min(bound, max(-(-total // count), total * weights[0] // sum(weights)))
    least = 1 if total - largest >= count - 1 else 0
    given, spare = [largest] + [least] * (count - 1), total - largest - least * (count - 1)
    while spare > 0:
        movable = [i for i in range(1, count) if given[i] < largest] or [i for i in range(1, count) if given[i] < bound]
        mass, left = sum([weights[i] for i in movable]), spare
        for i in movable:
            extra = min(bound - given[i], max(1, left * weights[i] // mass), spare)
            given[i] = given[i] + extra
            spare = spare - extra
    return np.array(given)


def centred(stream_key, dims, spread, bound, cuts=(), kind=jnp.bfloat16):
    drawn = jax.random.normal(stream_key, dims, jnp.float32) * spread
    if len(cuts) > 0:
        drawn = shard_levels(stream_key, dims, cuts, -0.22, 0.18) * drawn
    return jnp.clip(drawn, min=-bound, max=bound).astype(kind)


def setup_inputs(seed: int = 0) -> dict:
    splits = jax.random.split(jax.random.key(seed), 7)
    router_input = centred(splits[0], (TOKENS, D), 1.0, 6.0, ((0, 16), (1, 2)))
    router_weight = centred(splits[1], (D, EXPERTS), D ** -0.5, 0.125)
    expert_ids_keys = jax.random.split(jax.random.fold_in(splits[2], 1), TOKENS // TOK_DEV)
    expert_ids_turns = jax.random.permutation(jax.random.fold_in(splits[2], 3), TOKENS // TOK_DEV)
    expert_ids = jax.vmap(lambda own, number: deal_out(jax.random.fold_in(splits[2], 2), own, number, TOK_DEV, EXPERTS, TOPK, CAP, 2))(expert_ids_keys, expert_ids_turns).reshape((TOKENS, TOPK))
    down_weight = centred(splits[3], (EXPERTS * FF, D), FF ** -0.5, 0.0625, ((0, 8),))
    hidden = centred(splits[4], (N_DP, SOURCES * CAP, EXPERTS * FF), 1.0, 6.0, ((0, 4), (2, 8)))
    grad_output = centred(splits[5], (TOKENS, D), 0.25, 4.0, ((0, 32),))
    return dict(router_input=router_input, router_weight=router_weight, expert_ids=expert_ids, down_weight=down_weight, hidden=hidden, grad_output=grad_output)


def reference(router_input, router_weight, expert_ids, down_weight, hidden, grad_output):
    logits = jnp.dot(router_input, router_weight, preferred_element_type=jnp.float32)
    labels = jnp.arange(EXPERTS, dtype=jnp.int32)
    onehot_int = (expert_ids[:, :, None] == labels).astype(jnp.int32)
    onehot = onehot_int.astype(jnp.float32)
    picked = jnp.sum(onehot * logits[:, None, :], axis=2)
    first_gate = jax.nn.sigmoid(picked[:, 0] - picked[:, 1])
    second_gate = jax.nn.sigmoid(picked[:, 1] - picked[:, 0])
    gate_values = jnp.stack([first_gate, second_gate], axis=1)
    gate_low = gate_values.astype(jnp.bfloat16)
    blocks = TOKENS // TOK_DEV
    flat_hits = onehot_int.reshape(blocks, TOK_DEV * TOPK, EXPERTS)
    before = jnp.cumsum(flat_hits, axis=1) - flat_hits
    slot_pos = jnp.sum(before * flat_hits, axis=2).reshape(blocks, TOK_DEV, TOPK)
    slot_ids = jnp.arange(CAP, dtype=jnp.int32)
    dispatch_table = onehot.reshape(blocks, TOK_DEV, TOPK, EXPERTS, 1) * (slot_pos[:, :, :, None, None] == slot_ids).astype(jnp.float32)
    table_groups = dispatch_table.reshape(N_DP, SOURCES, TOK_DEV, TOPK, EXPERTS, CAP)
    grad_groups = grad_output.reshape(N_DP, SOURCES, TOK_DEV, D)
    gate_groups = gate_low.reshape(N_DP, SOURCES, TOK_DEV, TOPK)
    expert_weights = down_weight.reshape(EXPERTS, FF, D)

    def one_expert(pieces):
        expert_grad, expert_gate, expert_hidden, expert_weight = pieces
        expert_image = jnp.dot(expert_grad, expert_weight.T, preferred_element_type=jnp.float32)
        hidden_part = (expert_gate[:, None] * expert_image).astype(jnp.bfloat16)
        gate_part = jnp.sum(expert_hidden.astype(jnp.float32) * expert_image, axis=1)
        gated = (expert_gate[:, None] * expert_grad.astype(jnp.float32)).astype(jnp.bfloat16)
        weight_term = jnp.dot(expert_hidden.T, gated, preferred_element_type=jnp.float32).astype(jnp.bfloat16)
        return hidden_part, gate_part, weight_term

    def one_group(running_total, pieces):
        table_i, grad_i, gate_i, hidden_i = pieces
        slot_table = jnp.sum(table_i, axis=2)
        packed_grad = jnp.einsum("srec,srd->escd", slot_table, grad_i.astype(jnp.float32))
        packed_grad = packed_grad.astype(jnp.bfloat16).reshape(EXPERTS, SOURCES * CAP, D)
        packed_gate = jnp.einsum("srkec,srk->esc", table_i, gate_i.astype(jnp.float32)).reshape(EXPERTS, SOURCES * CAP)
        hidden_split = hidden_i.reshape(SOURCES * CAP, EXPERTS, FF).transpose(1, 0, 2)
        hidden_part, gate_part, weight_term = lax.map(one_expert, (packed_grad, packed_gate, hidden_split, expert_weights))
        running_total = running_total + weight_term.reshape(EXPERTS * FF, D).astype(jnp.float32)
        token_grad = jnp.einsum("srkec,esc->srk", table_i, gate_part.reshape(EXPERTS, SOURCES, CAP))
        hidden_rows = hidden_part.transpose(1, 0, 2).reshape(SOURCES * CAP, EXPERTS * FF)
        return running_total, (hidden_rows, token_grad)

    zero_total = jnp.zeros((EXPERTS * FF, D), jnp.float32)
    running_total, outputs = lax.scan(one_group, zero_total, (table_groups, grad_groups, gate_groups, hidden))
    hidden_grad, token_grad = outputs
    weight_grad = running_total.astype(jnp.bfloat16)
    gate_grad = token_grad.reshape(TOKENS, TOPK)
    mixed_term = jnp.sum(gate_values * gate_grad, axis=1, keepdims=True)
    logit_part = gate_values * (gate_grad - mixed_term)
    logit_grad = jnp.sum(onehot * logit_part[:, :, None], axis=1)
    input_grad = jnp.dot(logit_grad, router_weight.astype(jnp.float32).T, precision=lax.Precision.HIGHEST).astype(jnp.bfloat16)
    router_grad = jnp.dot(router_input.astype(jnp.float32).T, logit_grad, precision=lax.Precision.HIGHEST)
    return weight_grad, hidden_grad, router_grad, input_grad
```

```python
import functools

import jax
import jax.numpy as jnp
from jax import lax
from jax.experimental import pallas as pl
from jax.experimental.pallas import tpu as pltpu
from jax.sharding import PartitionSpec as P


def is_pow2(n):
    return n & (n - 1) == 0


def peer_perm(n, r):
    if is_pow2(n):
        return [(j, j ^ r) for j in range(n)]
    return [(j, (j + r) % n) for j in range(n)]


def peer_target(i, n, r):
    return i ^ r if is_pow2(n) else (i + r) % n


def gather_order(n):
    if not is_pow2(n):
        return list(range(n))
    order, bit = [0], n // 2
    while bit:
        order = order + [r ^ bit for r in order]
        bit //= 2
    return order


def gather_rows(x, axis):
    n = lax.axis_size(axis)
    if not is_pow2(n):
        return jnp.concatenate([x] + [lax.ppermute(x, axis, peer_perm(n, r)) for r in range(1, n)], axis=0)
    bit = n // 2
    while bit:
        far = lax.ppermute(x, axis, peer_perm(n, bit))
        x = jnp.concatenate([x, far], axis=0)
        bit = bit // 2
    return x


def sum_over(x, axis):
    n = lax.axis_size(axis)
    low = x.astype(jnp.bfloat16)
    parts = [lax.ppermute(low, axis, peer_perm(n, r)) for r in range(1, n)]
    total = low.astype(jnp.float32)
    for p in parts:
        total = total + p.astype(jnp.float32)
    return total


def features_of_own_rows(x, axis):
    n = lax.axis_size(axis)
    i = lax.axis_index(axis)
    blocks = x.reshape(n, x.shape[0] // n, x.shape[1])
    take = lambda b: lax.dynamic_index_in_dim(blocks, b, 0, keepdims=False)
    parts = [take(i)] + [
        lax.ppermute(take(peer_target(i, n, r)), axis, peer_perm(n, r)) for r in range(1, n)
    ]
    if n == 1:
        return parts[0]
    if n == 2:
        low = jnp.where(i == 0, parts[0], parts[1])
        high = jnp.where(i == 0, parts[1], parts[0])
        return jnp.concatenate([low, high], axis=1)
    stacked = jnp.stack(parts)
    ordered = [
        lax.dynamic_index_in_dim(stacked, (i ^ h) if is_pow2(n) else (i - h) % n, 0, keepdims=False)
        for h in range(n)
    ]
    return jnp.concatenate(ordered, axis=1)


def image_kernel(steps, rows_step, x_ref, gate_ref, w_hbm, h_hbm, o_hbm, acc_ref, wb, hb, ob, ws, hs, os):
    def w_copy(i):
        return pltpu.make_async_copy(w_hbm.at[pl.ds(i * rows_step, rows_step)], wb.at[i], ws.at[i])

    def h_copy(i):
        return pltpu.make_async_copy(h_hbm.at[:, pl.ds(i * rows_step, rows_step)], hb.at[i], hs.at[i])

    def o_copy(i):
        return pltpu.make_async_copy(ob.at[i], o_hbm.at[:, pl.ds(i * rows_step, rows_step)], os.at[i])

    def begin(i, carry):
        w_copy(i).start()
        h_copy(i).start()
        return carry

    lax.fori_loop(0, steps, begin, 0)
    acc_ref[...] = jnp.zeros_like(acc_ref)

    def step(i, carry):
        w_copy(i).wait()
        h_copy(i).wait()
        image = lax.dot_general(
            wb[i], x_ref[...], (((1,), (1,)), ((), ())), preferred_element_type=jnp.float32
        ).T
        ob[i] = (gate_ref[...] * image).astype(jnp.bfloat16)
        o_copy(i).start()
        prod = hb[i].astype(jnp.float32) * image
        total = prod[:, :128]
        for k in range(1, rows_step // 128):
            total = total + prod[:, k * 128 : (k + 1) * 128]
        acc_ref[...] += total
        return carry

    lax.fori_loop(0, steps, step, 0)

    def finish(i, carry):
        o_copy(i).wait()
        return carry

    lax.fori_loop(0, steps, finish, 0)


def expert_image(recv_grad, recv_gate, down_weight, hidden_rows):
    rows, width = recv_grad.shape
    units = down_weight.shape[0]
    rows_step = max(c for c in range(128, 1281, 128) if units % c == 0)
    steps = units // rows_step
    return pl.pallas_call(
        functools.partial(image_kernel, steps, rows_step),
        in_specs=[
            pl.BlockSpec(memory_space=pltpu.VMEM),
            pl.BlockSpec(memory_space=pltpu.VMEM),
            pl.BlockSpec(memory_space=pl.ANY),
            pl.BlockSpec(memory_space=pl.ANY),
        ],
        out_specs=[pl.BlockSpec(memory_space=pl.ANY), pl.BlockSpec(memory_space=pltpu.VMEM)],
        out_shape=[
            jax.ShapeDtypeStruct((rows, units), jnp.bfloat16),
            jax.ShapeDtypeStruct((rows, 128), jnp.float32),
        ],
        scratch_shapes=[
            pltpu.VMEM((steps, rows_step, width), jnp.bfloat16),
            pltpu.VMEM((steps, rows, rows_step), jnp.bfloat16),
            pltpu.VMEM((steps, rows, rows_step), jnp.bfloat16),
            pltpu.SemaphoreType.DMA((steps,)),
            pltpu.SemaphoreType.DMA((steps,)),
            pltpu.SemaphoreType.DMA((steps,)),
        ],
        compiler_params=pltpu.CompilerParams(vmem_limit_bytes=50 * 2**20),
        cost_estimate=pl.CostEstimate(
            flops=2 * rows * units * width,
            bytes_accessed=2 * units * (width + 2 * rows),
            transcendentals=0,
        ),
        name="expert_image",
    )(recv_grad, recv_gate, down_weight, hidden_rows)


def device_step(router_input, router_weight, expert_ids, down_weight, hidden, grad_output):
    token_rows, model_width = grad_output.shape
    expert_count = router_weight.shape[1]
    choose_count = expert_ids.shape[1]
    ranks = ("expert", "tensor")
    sources = lax.axis_size("expert") * lax.axis_size("tensor")
    spread = sources // expert_count
    groups = lax.axis_size("dp")
    group = lax.axis_index("dp")
    capacity = hidden.shape[1] // sources
    hidden_rows = hidden[0]
    units_own = hidden_rows.shape[1] // groups
    whole_gather = groups * hidden_rows.shape[0] * model_width <= 2**21

    take_units = lambda g: lax.dynamic_slice_in_dim(hidden_rows, g * units_own, units_own, axis=1)
    hidden_parts = [
        lax.ppermute(take_units(peer_target(group, groups, r)), "dp", peer_perm(groups, r)) if r else take_units(group)
        for r in (gather_order(groups) if whole_gather else range(groups))
    ]

    full_input = features_of_own_rows(router_input, "tensor")
    logits = jnp.dot(full_input, router_weight, preferred_element_type=jnp.float32)
    labels = jnp.arange(expert_count, dtype=jnp.int32)
    onehot_int = (expert_ids[:, :, None] == labels).astype(jnp.int32)
    onehot = onehot_int.astype(jnp.float32)
    picked = jnp.sum(onehot * logits[:, None, :], axis=2)
    first_gate = jax.nn.sigmoid(picked[:, 0] - picked[:, 1])
    second_gate = jax.nn.sigmoid(picked[:, 1] - picked[:, 0])
    gate_values = jnp.stack([first_gate, second_gate], axis=1)
    gate_low = gate_values.astype(jnp.bfloat16)

    flat_hits = onehot_int.reshape(token_rows * choose_count, expert_count)
    earlier = jnp.tril(jnp.ones((token_rows * choose_count,) * 2, jnp.bfloat16), -1)
    before = jnp.dot(earlier, flat_hits.astype(jnp.bfloat16), preferred_element_type=jnp.float32)
    slot_pos = jnp.sum(before * flat_hits, axis=1).astype(jnp.int32).reshape(token_rows, choose_count)
    slot_ids = jnp.arange(capacity, dtype=jnp.int32)
    dispatch_table = onehot[:, :, :, None] * (slot_pos[:, :, None, None] == slot_ids).astype(jnp.float32)
    slot_table = jnp.sum(dispatch_table, axis=1).reshape(token_rows, expert_count * capacity)
    packed_grad = lax.dot_general(
        slot_table.astype(jnp.bfloat16), grad_output, (((0,), (0,)), ((), ())),
        preferred_element_type=jnp.float32,
    ).astype(jnp.bfloat16)
    packed_gate = jnp.sum(
        dispatch_table * gate_low.astype(jnp.float32)[:, :, None, None], axis=(0, 1)
    ).astype(jnp.bfloat16)

    lanes = 128
    lines = capacity * model_width // lanes
    gate_lines = -(-capacity // lanes) * 8
    send_grad = packed_grad.reshape(expert_count, lines, lanes)
    send_gate = jnp.pad(packed_gate, ((0, 0), (0, gate_lines * lanes - capacity))).reshape(
        expert_count, gate_lines, lanes
    )
    send = jnp.repeat(jnp.concatenate([send_grad, send_gate], axis=1), spread, axis=0)
    recv = lax.all_to_all(send, ranks, split_axis=0, concat_axis=0, tiled=True)
    recv_grad = recv[:, :lines].reshape(sources * capacity, model_width)
    recv_gate = (
        recv[:, lines:].reshape(sources, gate_lines * lanes)[:, :capacity]
        .reshape(sources * capacity, 1)
        .astype(jnp.float32)
    )
    gated_grad = (recv_gate * recv_grad.astype(jnp.float32)).astype(jnp.bfloat16)
    gated_all = gather_rows(gated_grad, "dp") if whole_gather else None

    hidden_part, partial_lanes = expert_image(recv_grad, recv_gate, down_weight, hidden_rows)
    gate_partial = jnp.sum(partial_lanes, axis=1).reshape(sources, 1, capacity)
    returned = lax.all_to_all(gate_partial, ranks, split_axis=0, concat_axis=0, tiled=True)
    expert_sums = jnp.sum(returned.reshape(expert_count, spread, capacity), axis=1)
    gate_grad = jnp.sum(dispatch_table * expert_sums, axis=(2, 3))
    mixed_term = jnp.sum(gate_values * gate_grad, axis=1, keepdims=True)
    logit_part = gate_values * (gate_grad - mixed_term)
    logit_grad = jnp.sum(onehot * logit_part[:, :, None], axis=1)
    input_grad = jnp.dot(
        logit_grad, router_weight.astype(jnp.float32).T, precision=lax.Precision.HIGHEST
    ).astype(jnp.bfloat16)
    router_part = lax.dot_general(
        logit_grad, full_input.astype(jnp.float32), (((0,), (0,)), ((), ())),
        precision=lax.Precision.HIGHEST,
    )
    for axis in ("tensor", "dp", "expert"):
        router_part = sum_over(router_part, axis)
    rows_dims = (((0,), (0,)), ((), ()))
    if whole_gather:
        hidden_all, gated_all = lax.optimization_barrier((jnp.concatenate(hidden_parts, axis=0), gated_all))
        weight_sum = lax.dot_general(hidden_all, gated_all, rows_dims, preferred_element_type=jnp.float32)
    else:
        weight_sum, gated = 0.0, gated_grad
        for r in range(groups):
            if r:
                gated, _ = lax.optimization_barrier((gated_grad, weight_sum))
                gated = lax.ppermute(gated, "dp", peer_perm(groups, r))
            weight_sum += lax.dot_general(hidden_parts[r], gated, rows_dims, preferred_element_type=jnp.float32)
    weight_sum = weight_sum.astype(jnp.bfloat16)
    return weight_sum, hidden_part[None], router_part.T, input_grad


def solution(mesh):
    return jax.shard_map(
        device_step,
        mesh=mesh,
        in_specs=(
            P(("dp", "expert"), "tensor"),
            P(),
            P(("dp", "expert", "tensor"), None),
            P(("expert", "tensor"), None),
            P("dp", None, ("expert", "tensor")),
            P(("dp", "expert", "tensor"), None),
        ),
        out_specs=(
            P(("expert", "tensor", "dp"), None),
            P("dp", None, ("expert", "tensor")),
            P(),
            P(("dp", "expert", "tensor"), None),
        ),
        check_vma=False,
    )
```
